512 devices in a mesh: member: 2 (over y), lat: 32 (over z), lon: 4 (over x), lev: 2 (over core).
Axes of the slice: x: 4, y: 2, z: 32, core: 2. Of those that a mesh axis runs over, the one named last changes fastest.
The devices are a block of a 4x16x32 slice.
Arguments:
- perturbation: bfloat16 [4, 64, 128, 16, 128], P('member', 'lev', 'lat', 'lon'), parts along dimension 0, may hold values from -6 to 6
- adjoint_forcing: bfloat16 [4, 64, 128, 16, 128], P('member', 'lev', 'lat', 'lon'), parts along dimension 0, may hold values from -6 to 6
- source_rows: int32 [128, 16, 4], P('lat', 'lon'), may hold values from 0 to 127, as said below
- source_cols: int32 [128, 16, 4], P('lat', 'lon'), may hold values from 0 to 15, as said below
- cubic_weights: bfloat16 [128, 16, 4, 128, 128], P('lat', 'lon'), may hold values from -1.5 to 1.5
Outputs:
- tangent_out: bfloat16 [4, 64, 128, 16, 128], P('member', 'lev', 'lat', 'lon'), parts along dimension 0
- adjoint_out: bfloat16 [4, 64, 128, 16, 128], P('member', 'lev', 'lat', 'lon'), parts along dimension 0
The draws below stay inside these ranges and needn't reach their ends.
There are 2 independent parts, one for each index of `member`. The reference program is written for one: setup_inputs(seed, part) draws one part's arguments, and reference() takes and returns one part's arrays. A program takes and returns all parts, laid end to end along the dimension named above; an argument that names none is the same for every part. Nothing has to cross between parts.
Inputs may be any that keep to these rules, and one draw needn't show every extreme that they name: source_rows[i, j, k] differs from i by at most 8. source_cols[i, j, k] is j + d modulo 16 with d from -1 to 1, and from -2 to 2 where i lies in the first or last 4 block rows.
All inputs are finite; a program needn't handle non-finite values.
Results may differ from the reference program's by a relative error of at most 0.004.
Values may be sent and summed in bfloat16 or wider, within the bound.
No kernel may reach another device: no remote copies, remote signals or barrier semaphores. Data moves between devices by JAX's collectives and lax.ppermute only.
A program may use at most 64 MiB of HBM per device.

```python
import math
import jax
import jax.numpy as jnp
from jax import lax

CELLS = 128
STENCIL = 4
BAND_ROWS = 4
FIELDS = 2
LEVELS = 64
LAT_ROWS = 128
LON_COLS = 16
N_LAT = 32


def draw_source_rows(key, part):
    first_key, second_key = jax.random.split(jax.random.fold_in(key, 11))
    row_ids = jnp.arange(LAT_ROWS, dtype=jnp.int32)[:, None, None]
    reach_rows = 2 * BAND_ROWS
    shape = (LAT_ROWS, LON_COLS, STENCIL)
    offsets = jax.random.randint(first_key, shape, -reach_rows, reach_rows + 1)
    signs = 2 * jax.random.randint(second_key, shape, 0, 2) - 1
    last_one = jnp.arange(STENCIL, dtype=jnp.int32)[None, None, :] == STENCIL - 1
    offsets = jnp.where(last_one, signs * reach_rows, offsets)
    return jnp.clip(row_ids + offsets, 0, LAT_ROWS - 1).astype(jnp.int32)


def draw_source_cols(key, part):
    first_key, second_key = jax.random.split(jax.random.fold_in(key, 23))
    row_ids = jnp.arange(LAT_ROWS, dtype=jnp.int32)[:, None, None]
    band_ids = row_ids // BAND_ROWS
    polar = (band_ids == 0) | (band_ids == N_LAT - 1)
    reach_cols = jnp.where(polar, 2, 1)
    col_ids = jnp.arange(LON_COLS, dtype=jnp.int32)[None, :, None]
    shape = (LAT_ROWS, LON_COLS, STENCIL)
    offsets = jax.random.randint(first_key, shape, -2, 3)
    offsets = jnp.clip(offsets, -reach_cols, reach_cols)
    signs = 2 * jax.random.randint(second_key, shape, 0, 2) - 1
    last_one = jnp.arange(STENCIL, dtype=jnp.int32)[None, None, :] == STENCIL - 1
    offsets = jnp.where(last_one & polar, signs * 2, offsets)
    return jnp.mod(col_ids + offsets, LON_COLS).astype(jnp.int32)


def draw_cubic_weights(key, part):
    second_key = jax.random.fold_in(jax.random.fold_in(key, 37), 1)
    identity = jnp.eye(CELLS, dtype=jnp.float32)
    diagonal = jnp.full((LAT_ROWS, LON_COLS, STENCIL, 1, 1), 0.5, jnp.float32)
    noise = jax.random.normal(second_key, (LAT_ROWS, LON_COLS, STENCIL, CELLS, CELLS), jnp.float32)
    noise = jnp.clip(noise * (0.35 / math.sqrt(CELLS)), -0.6, 0.6)
    return (diagonal * identity + noise).astype(jnp.bfloat16)


def steps_of(rng, shape, shards, least, largest):
    loudness, own = 1.0, jax.random.fold_in(rng, 6)
    for axis_at, blocks in shards:
        draws = jnp.exp(jax.random.uniform(jax.random.fold_in(own, axis_at), (blocks,), jnp.float32, least / len(shards), largest / len(shards)))
        loudness = loudness * jnp.repeat(draws, shape[axis_at] // blocks).reshape([-1 if axis == axis_at else 1 for axis in range(len(shape))])
    return loudness


def centred(key, shape, scale, reach, cuts=(), kind=jnp.bfloat16):
    drawn = scale * jax.random.normal(key, shape, jnp.float32)
    if cuts:
        drawn = drawn * steps_of(key, shape, cuts, -0.22, 0.18)
    return jnp.clip(drawn, -reach, reach).astype(kind)


def setup_inputs(seed: int = 0, part: int = 0) -> dict:
    arg_keys = jax.random.split(jax.random.key(seed), 6)
    part_splits = jax.random.split(jax.random.fold_in(arg_keys[5], part), 6)
    return {
        "perturbation": centred(part_splits[0], (FIELDS, LEVELS, LAT_ROWS, LON_COLS, CELLS), 1.0, 6.0, ((1, 2), (2, 32), (3, 4))),
        "adjoint_forcing": centred(part_splits[1], (FIELDS, LEVELS, LAT_ROWS, LON_COLS, CELLS), 1.0, 6.0, ((1, 2), (2, 32), (3, 4))),
        "source_rows": draw_source_rows(jax.random.fold_in(arg_keys[5], 71), part),
        "source_cols": draw_source_cols(jax.random.fold_in(arg_keys[5], 71), part),
        "cubic_weights": draw_cubic_weights(jax.random.fold_in(arg_keys[5], 71), part),
    }


def interpolate(field, source_rows, source_cols, cubic_weights):

    def one_row(pieces):
        rows_here, cols_here, weights_here = pieces
        picked = field[:, :, rows_here, cols_here, :]
        return jnp.einsum('flnks,nksc->flnc', picked, weights_here.astype(jnp.float32), precision=lax.Precision.HIGHEST)
    mapped = lax.map(one_row, (source_rows, source_cols, cubic_weights))
    return jnp.transpose(mapped, (1, 2, 0, 3, 4))

def reference(perturbation, adjoint_forcing, source_rows, source_cols, cubic_weights):

    def linear_map(field):
        return interpolate(field, source_rows, source_cols, cubic_weights)
    tangent, pullback = jax.vjp(linear_map, perturbation.astype(jnp.float32))
    adjoint = pullback(adjoint_forcing.astype(jnp.float32))[0]
    return (tangent.astype(jnp.bfloat16), adjoint.astype(jnp.bfloat16))
```

```python
import functools

import jax
import jax.numpy as jnp
from jax import lax
from jax.experimental import pallas as pl
from jax.experimental.pallas import tpu as pltpu
from jax.sharding import PartitionSpec as P

VMEM = pl.BlockSpec(memory_space=pltpu.VMEM)
SMEM = pl.BlockSpec(memory_space=pltpu.SMEM)
ANY = pl.BlockSpec(memory_space=pl.ANY)
PARAMS = pltpu.CompilerParams(vmem_limit_bytes=6 << 20)


def passed_along(array, axis, by):
    devices = lax.axis_size(axis)
    pairs = [(i, i + by) for i in range(devices) if 0 <= i + by < devices]
    return lax.ppermute(array, axis, pairs)


def shifted(array, axis, by):
    devices = lax.axis_size(axis)
    return lax.ppermute(array, axis, [(i, (i + by) % devices) for i in range(devices)])


def adjoint_kernel(tile_cols, height, slots, pos_ref, forcing_ref, weights_ref, acc_ref, west_ref, east_ref):
    targets, stencil, cells, _ = weights_ref.shape
    inner = height * tile_cols
    acc_ref[...] = jnp.zeros_like(acc_ref)
    for t in range(targets):
        part = lax.dot_general(
            forcing_ref[t],
            weights_ref[t].reshape(stencil * cells, cells),
            (((1,), (1,)), ((), ())),
            preferred_element_type=jnp.float32,
        )
        for k in range(stencil):
            place = pos_ref[t * stencil + k]
            acc_ref[place] += part[:, k * cells : (k + 1) * cells]
    west_ref[...] = acc_ref[inner : inner + slots].astype(west_ref.dtype)
    east_ref[...] = acc_ref[inner + slots : inner + 2 * slots].astype(east_ref.dtype)


def edges_kernel(tile_cols, band_rows, slots, acc_ref, west_ref, east_ref, polar_ref, *out_refs):
    height = 5 * band_rows
    polar = polar_ref[0] != 0
    last = tile_cols - 1
    for r in range(height):
        out = out_refs[r // band_rows]
        row = (r % band_rows) * tile_cols
        second = (r + slots // 2) % slots
        from_west, from_east = west_ref[r].astype(jnp.float32), east_ref[r].astype(jnp.float32)
        for c in range(tile_cols):
            value = acc_ref[r * tile_cols + c]
            if c == 0:
                value = value + from_west
            if c == last:
                value = value + from_east
            if c == 1:
                value = value + jnp.where(polar, west_ref[second].astype(jnp.float32), 0.0)
            if c == last - 1:
                value = value + jnp.where(polar, east_ref[second].astype(jnp.float32), 0.0)
            out[row + c] = value.astype(out.dtype)


def pack_kernel(tile_cols, band_rows, slots, side_ref, *refs):
    bands, (west_ref, east_ref) = refs[:5], refs[5:]
    height, half = 5 * band_rows, slots // 2
    last = tile_cols - 1

    def block(r, c):
        return bands[r // band_rows][(r % band_rows) * tile_cols + c]

    for r in range(height):
        west_ref[r] = block(r, 0)
        east_ref[r] = block(r, last)
    for r in range(height, slots):
        west_ref[r] = block(0, 0)
        east_ref[r] = block(0, last)

    @pl.when(side_ref[0] == 1)
    def _():
        for r in range(height - half, height):
            west_ref[(r + half) % slots] = block(r, 1)
            east_ref[(r + half) % slots] = block(r, last - 1)

    @pl.when(side_ref[0] == 2)
    def _():
        for r in range(half):
            west_ref[(r + half) % slots] = block(r, 1)
            east_ref[(r + half) % slots] = block(r, last - 1)


def tangent_kernel(pos_ref, weights_ref, *refs):
    sources, out_ref, seen, sems = refs[:-3], refs[-3], refs[-2], refs[-1]
    targets, stencil, cells, _ = weights_ref.shape
    copies, at = [], 0
    for n, source in enumerate(sources):
        size = source.shape[0]
        copies.append(pltpu.make_async_copy(source, seen.at[pl.ds(at, size)], sems.at[n]))
        at += size
    for copy in copies:
        copy.start()
    for copy in copies:
        copy.wait()
    for t in range(targets):
        picked = [seen[pos_ref[t * stencil + k]] for k in range(stencil)]
        out_ref[t] = jnp.dot(
            jnp.concatenate(picked, axis=1),
            weights_ref[t].reshape(stencil * cells, cells),
            preferred_element_type=jnp.float32,
        ).astype(out_ref.dtype)


def on_device(perturbation, adjoint_forcing, source_rows, source_cols, cubic_weights):
    fields, levels, band_rows, tile_cols, cells = perturbation.shape
    stencil = source_rows.shape[2]
    rows = fields * levels
    targets = band_rows * tile_cols
    reach = 2 * band_rows
    height = band_rows + 2 * reach
    half = height - reach
    slots = 2 * half
    inner = height * tile_cols
    places = inner + 2 * slots
    bf16, f32 = jnp.bfloat16, jnp.float32

    band_index, tile_index = lax.axis_index("lat"), lax.axis_index("lon")
    first, final = band_index == 0, band_index == lax.axis_size("lat") - 1
    side = jnp.where(first, 1, jnp.where(final, 2, 0)).astype(jnp.int32).reshape(1)
    total_cols = tile_cols * lax.axis_size("lon")

    local_rows = source_rows - band_index * band_rows + reach
    local_cols = jnp.mod(source_cols - tile_index * tile_cols + 2, total_cols) - 2
    near = (local_cols == -1) | (local_cols == tile_cols)
    slot = jnp.where(near, local_rows, (local_rows + half) % slots)
    positions = jnp.where(
        (local_cols >= 0) & (local_cols < tile_cols),
        local_rows * tile_cols + local_cols,
        inner + slot + jnp.where(local_cols < 0, 0, slots),
    ).reshape(-1)

    def blocks_first(x):
        return jnp.transpose(x, (2, 3, 0, 1, 4)).reshape(targets, rows, cells)

    def blocks_last(x):
        return jnp.transpose(x.reshape(band_rows, tile_cols, fields, levels, cells), (2, 3, 0, 1, 4))

    weights = cubic_weights.reshape(targets, stencil, cells, cells)
    flops = 2 * rows * targets * stencil * cells * cells

    def shape(n, dtype=bf16):
        return jax.ShapeDtypeStruct((n, rows, cells), dtype)

    own = blocks_first(perturbation)
    lower_far = passed_along(own, "lat", 2)
    upper_far = passed_along(own, "lat", -2)

    forcing = blocks_first(adjoint_forcing)
    acc, west_part, east_part = pl.pallas_call(
        functools.partial(adjoint_kernel, tile_cols, height, slots),
        out_shape=(shape(places, f32), shape(slots), shape(slots)),
        in_specs=[SMEM, VMEM, VMEM],
        out_specs=(VMEM, VMEM, VMEM),
        compiler_params=PARAMS,
        cost_estimate=pl.CostEstimate(flops=flops, bytes_accessed=8 << 20, transcendentals=0),
        name="adjoint",
    )(positions, forcing, weights)
    from_east = shifted(west_part, "lon", -1)
    from_west = shifted(east_part, "lon", 1)

    lower_near = passed_along(own, "lat", 1)
    upper_near = passed_along(own, "lat", -1)

    to_lower_far, to_lower_near, kept, to_upper_near, to_upper_far = pl.pallas_call(
        functools.partial(edges_kernel, tile_cols, band_rows, slots),
        out_shape=(shape(targets), shape(targets), shape(targets, f32), shape(targets), shape(targets)),
        in_specs=[VMEM, VMEM, VMEM, SMEM],
        out_specs=(VMEM,) * 5,
        compiler_params=PARAMS,
        cost_estimate=pl.CostEstimate(flops=flops // 4, bytes_accessed=8 << 20, transcendentals=0),
        name="edges",
    )(acc, from_west, from_east, side)
    got = [
        passed_along(to_lower_far, "lat", -2),
        passed_along(to_upper_far, "lat", 2),
        passed_along(to_lower_near, "lat", -1),
        passed_along(to_upper_near, "lat", 1),
    ]

    bands = (lower_far, lower_near, own, upper_near, upper_far)
    west_strip, east_strip = pl.pallas_call(
        functools.partial(pack_kernel, tile_cols, band_rows, slots),
        out_shape=(shape(slots), shape(slots)),
        in_specs=[SMEM] + [VMEM] * 5,
        out_specs=(VMEM, VMEM),
        compiler_params=PARAMS,
        cost_estimate=pl.CostEstimate(flops=flops // 4, bytes_accessed=2 << 20, transcendentals=0),
        name="pack",
    )(side, *bands)
    east = shifted(west_strip, "lon", -1)
    west = shifted(east_strip, "lon", 1)
    tangent = pl.pallas_call(
        tangent_kernel,
        out_shape=shape(targets),
        in_specs=[SMEM, VMEM] + [ANY] * 7,
        out_specs=VMEM,
        scratch_shapes=[pltpu.VMEM((places, rows, cells), bf16), pltpu.SemaphoreType.DMA((7,))],
        compiler_params=PARAMS,
        cost_estimate=pl.CostEstimate(flops=flops, bytes_accessed=5 << 20, transcendentals=0),
        name="tangent",
    )(positions, weights, *bands, west, east)
    tangent_out = blocks_last(tangent)

    adjoint = kept
    for part in got:
        adjoint = adjoint + part.astype(f32)
    return (tangent_out, blocks_last(adjoint.astype(bf16)))


def solution(mesh):
    placed = (
        P("member", "lev", "lat", "lon", None),
        P("member", "lev", "lat", "lon", None),
        P("lat", "lon", None),
        P("lat", "lon", None),
        P("lat", "lon", None, None, None),
    )
    return jax.shard_map(
        on_device,
        mesh=mesh,
        in_specs=placed,
        out_specs=(P("member", "lev", "lat", "lon", None), P("member", "lev", "lat", "lon", None)),
        check_vma=False,
    )
```
